32 devices in a mesh: dp: 4 (over x, core), ctx: 8 (over z, y).
Axes of the slice: x: 2, y: 2, z: 4, core: 2. Of those that a mesh axis runs over, the one named last changes fastest.
Arguments:
- tokens: bfloat16 [4096, 1792], P(('dp', 'ctx')), may hold values from -6 to 6
- cotangent: bfloat16 [4096, 1792], P(('dp', 'ctx')), may hold values from -6 to 6
- expert_ids: int32 [4096, 4], P(('dp', 'ctx')), may hold values from 0 to 15, all different within a row; in each aligned block of 128 rows (0 to 127, 128 to 255, ...) at most 40 rows name the same one
- norm_gain: float32 [1792], replicated, may hold values from 0.5 to 1.5
- router_weight: bfloat16 [1792, 16], replicated, may hold values from -0.125 to 0.125
- gate_weight: bfloat16 [16, 1792, 1536], P('ctx', None, 'dp'), may hold values from -0.125 to 0.125
- up_weight: bfloat16 [16, 1792, 1536], P('ctx', None, 'dp'), may hold values from -0.125 to 0.125
- down_weight: bfloat16 [16, 1536, 1792], P('ctx', 'dp'), may hold values from -0.15625 to 0.15625
Outputs:
- grad_tokens: bfloat16 [4096, 1792], P(('dp', 'ctx'))
- grad_gate: bfloat16 [16, 1792, 1536], P('ctx', None, 'dp')
- grad_up: bfloat16 [16, 1792, 1536], P('ctx', None, 'dp')
- grad_down: bfloat16 [16, 1536, 1792], P('ctx', 'dp')
- grad_router: float32 [1792, 16], P(('dp', 'ctx'))
- grad_gain: float32 [1792], P(('dp', 'ctx'))
The draws below stay inside these ranges and needn't reach their ends.
Inputs may be any that keep to these rules, and one draw needn't show every extreme that they name: `expert_ids`: each row names 4 different experts; among the rows of one device no expert is named more than 40 times.
All inputs are finite; a program needn't handle non-finite values.
Results may differ from the reference program's by a relative error of at most 0.02.
Values may be sent and summed in bfloat16 or wider, within the bound.
No kernel may reach another device: no remote copies, remote signals or barrier semaphores. Data moves between devices by JAX's collectives and lax.ppermute only.
A program may use at most 192 MiB of HBM per device.

```python
import math
import jax
import jax.numpy as jnp
import numpy as np
from jax import lax

D = 1792
FF = 1536
TOP = 4
TOK_DEV = 128
EXPERTS = 16
CAP = 40
TOKENS = 4096
N_DP = 4
N_CTX = 8


def raised(values, own_key, source, target, blocks, factor):
    def block_of(dim):
        return (jnp.arange(values.shape[dim]) // (values.shape[dim] // blocks)).reshape((-1,) + (1,) * (values.ndim - 1 - dim))

    near = jax.random.permutation(own_key, blocks)[block_of(target)]
    second = (block_of(target) + blocks // 2) % blocks
    return jnp.where((block_of(source) == near) | (block_of(source) == second), factor * values, values)


def block_scale(stream_key, shape, cuts, smallest, largest):
    gain, own = 1.0, jax.random.fold_in(stream_key, 6)
    for axis_at, shards_of in cuts:
        draws = jnp.exp(jax.random.uniform(jax.random.fold_in(own, axis_at), (shards_of,), jnp.float32, smallest / len(cuts), largest / len(cuts)))
        gain = gain * jnp.repeat(draws, shape[axis_at] // shards_of).reshape([-1 if axis == axis_at else 1 for axis in range(len(shape))])
    return gain


def shared_out(key, own, number, rows, count, top, bound, skew):
    order = jax.random.permutation(key, count)
    crowded, common = load_shares(count, rows * top, bound, skew, True), load_shares(count, rows * top, bound, skew, False)
    places = jnp.arange(count)

    def named(lengths, rotation):
        used = int((lengths > 0).sum())
        fixed = max(1, used // 4)
        moved = fixed + (places - fixed + rotation * (used - fixed)) % max(1, count - fixed)
        return jnp.zeros((count,), jnp.int32).at[order[jnp.where(places < fixed, places, moved)]].set(jnp.asarray(lengths, jnp.int32))

    lengths = jnp.where(number % 4 == 0, named(crowded, number // 4), named(common, number - number // 4 - 1))
    mixed = jax.random.permutation(jax.random.fold_in(own, 3), count)
    donor, taker = mixed[0:count // 2 * 2:2], mixed[1:count // 2 * 2:2]
    room = jnp.minimum(lengths[donor] - 1, bound - lengths[taker]) // 2
    room = jnp.where((donor == order[0]) | (taker == order[0]) | (lengths[taker] == 0), 0, jnp.maximum(room, 0))
    moved = jax.random.randint(jax.random.fold_in(own, 4), (count // 2,), 0, 1 << 20) % (room + 1)
    lengths = lengths.at[donor].add(-moved).at[taker].add(moved)
    items = jnp.searchsorted(jnp.cumsum(lengths), jnp.arange(rows * top), side="right").astype(jnp.int32)
    table = items.reshape(top, rows).T
    table = table[jax.random.permutation(jax.random.fold_in(own, 1), rows)]
    rotation = jax.random.randint(jax.random.fold_in(own, 2), (rows, 1), 0, top)
    return jnp.take_along_axis(table, (jnp.arange(top)[None, :] + rotation) % top, axis=1)


def load_shares(number_of, total, limit, lean, full):
    portions = [(1 << 20) // math.isqrt(rank ** lean) + 1 for rank in range(1, number_of + 1)]
    largest = limit if full else min(limit, max(-(-total // number_of), total * portions[0] // sum(portions)))
    least = 1 if total - largest >= number_of - 1 else 0
    counts, spare = [largest] + [least] * (number_of - 1), total - largest - least * (number_of - 1)
    while spare > 0:
        free = [i for i in range(1, number_of) if counts[i] < largest] or [i for i in range(1, number_of) if counts[i] < limit]
        pool, budget = sum([portions[i] for i in free]), spare
        for i in free:
            extra = min(limit - counts[i], max(1, budget * portions[i] // pool), spare)
            counts[i] = counts[i] + extra
            spare = spare - extra
    return np.array(counts)


def bell_draw(own_key, shape, width, most, pieces=(), held_as=jnp.bfloat16):
    gain = block_scale(own_key, shape, pieces, -0.22, 0.18) if pieces else 1.0
    result = jax.random.normal(own_key, shape, jnp.float32) * width * gain
    return jnp.minimum(jnp.maximum(result, -most), most).astype(held_as)


def gaussian_with(stream_key, shape, spread, limit, pieces, heavy, kind=jnp.bfloat16):
    values = spread * jax.random.normal(stream_key, shape, jnp.float32)
    if pieces:
        values = values * block_scale(stream_key, shape, pieces, -0.22, 0.18)
    return jnp.clip(raised(values, jax.random.fold_in(stream_key, 3), *heavy), -limit, limit).astype(kind)


def setup_inputs(seed: int = 0) -> dict:
    keys = jax.random.split(jax.random.key(seed), 9)
    tokens = gaussian_with(keys[0], (TOKENS, D), 1.0, 6.0, ((0, 32),), (0, 1, 32, 2.75))
    cotangent = bell_draw(keys[1], (TOKENS, D), 1.0, 6.0, ((0, 32),))
    expert_ids_keys = jax.random.split(jax.random.fold_in(keys[2], 1), TOKENS // TOK_DEV)
    expert_ids_turns = jax.random.permutation(jax.random.fold_in(keys[2], 3), TOKENS // TOK_DEV)
    expert_ids = jax.vmap(lambda own, number: shared_out(jax.random.fold_in(keys[2], 2), own, number, TOK_DEV, EXPERTS, TOP, CAP, 2))(expert_ids_keys, expert_ids_turns).reshape((TOKENS, TOP))
    norm_gain = jnp.clip(1.0 + 0.1 * jax.random.normal(keys[3], (D,), jnp.float32), 0.5, 1.5)
    router_weight = bell_draw(keys[4], (D, EXPERTS), D ** -0.5, 0.125)
    gate_weight = bell_draw(keys[5], (EXPERTS, D, FF), D ** -0.5, 0.125, ((0, 8), (2, 4)))
    up_weight = bell_draw(keys[6], (EXPERTS, D, FF), D ** -0.5, 0.125, ((0, 8), (2, 4)))
    down_weight = bell_draw(keys[7], (EXPERTS, FF, D), FF ** -0.5, 0.15625, ((0, 8), (1, 4)))
    return dict(tokens=tokens, cotangent=cotangent, expert_ids=expert_ids, norm_gain=norm_gain, router_weight=router_weight, gate_weight=gate_weight, up_weight=up_weight, down_weight=down_weight)


EPSILON = 1e-05
SWISH_SCALE = 1.702

def reference(tokens, cotangent, expert_ids, norm_gain, router_weight, gate_weight, up_weight, down_weight):
    ntoken = tokens.shape[0]
    widened = tokens.astype(jnp.float32)
    inverse = lax.rsqrt(lax.optimization_barrier(jnp.mean(widened * widened, axis=1, keepdims=True)) + EPSILON)
    scaled = widened * inverse
    normed = (scaled * norm_gain).astype(jnp.bfloat16)
    logits = jnp.dot(normed, router_weight, preferred_element_type=jnp.float32)
    chosen = jnp.take_along_axis(logits, expert_ids, axis=1)
    lifted = jnp.exp(chosen)
    gates = lifted / lax.optimization_barrier(jnp.sum(lifted, axis=1, keepdims=True))
    devices = N_DP * N_CTX
    per_device = TOK_DEV * TOP
    block_ids = expert_ids.reshape(devices, per_device)
    labels = jnp.arange(EXPERTS, dtype=jnp.int32)
    hits = (block_ids[:, :, None] == labels).astype(jnp.int32)
    rank = lax.optimization_barrier(jnp.sum((jnp.cumsum(hits, axis=1) - 1) * hits, axis=2))
    position = jnp.arange(devices, dtype=jnp.int32)[:, None] * CAP + rank
    assign = jnp.arange(devices * per_device, dtype=jnp.int32)
    flat_ids = block_ids.reshape(-1)
    flat_pos = position.reshape(-1).astype(jnp.int32)
    table = jnp.zeros((EXPERTS, devices * CAP), jnp.int32).at[flat_ids, flat_pos].set(assign)
    present_all = jnp.zeros((EXPERTS, devices * CAP), jnp.float32).at[flat_ids, flat_pos].set(1.0)
    gates_flat = gates.reshape(-1)

    def expert_step(carry, inputs):
        grad_tok, score_acc = carry
        entry, present, w_gate, w_up, w_down = inputs
        token = entry // TOP
        keep = present[:, None] > 0.0
        rows = jnp.where(keep, normed[token], jnp.zeros_like(normed[token]))
        upstream = jnp.where(keep, cotangent[token], jnp.zeros_like(cotangent[token]))
        weight = present * gates_flat[entry]
        gate_pre = jnp.dot(rows, w_gate, preferred_element_type=jnp.float32)
        up_pre = jnp.dot(rows, w_up, preferred_element_type=jnp.float32)
        squash = jax.nn.sigmoid(SWISH_SCALE * gate_pre)
        hidden = (gate_pre * squash * (up_pre + 1.0)).astype(jnp.bfloat16)
        grad_out = jnp.dot(upstream, w_down.T, preferred_element_type=jnp.float32)
        score = lax.optimization_barrier(jnp.sum(grad_out * hidden.astype(jnp.float32), axis=1))
        grad_hidden = weight[:, None] * grad_out
        slope = squash + SWISH_SCALE * gate_pre * squash * (1.0 - squash)
        grad_pre_gate = (grad_hidden * (up_pre + 1.0) * slope).astype(jnp.bfloat16)
        grad_pre_up = (grad_hidden * gate_pre * squash).astype(jnp.bfloat16)
        scaled_up = (weight[:, None] * upstream.astype(jnp.float32)).astype(jnp.bfloat16)
        down_grad = jnp.dot(hidden.T, scaled_up, preferred_element_type=jnp.float32).astype(jnp.bfloat16)
        gate_grad = jnp.dot(rows.T, grad_pre_gate, preferred_element_type=jnp.float32).astype(jnp.bfloat16)
        up_grad = jnp.dot(rows.T, grad_pre_up, preferred_element_type=jnp.float32).astype(jnp.bfloat16)
        back = jnp.dot(grad_pre_gate, w_gate.T, preferred_element_type=jnp.float32)
        back = back + jnp.dot(grad_pre_up, w_up.T, preferred_element_type=jnp.float32)
        grad_tok = grad_tok.at[token].add(back)
        score_acc = score_acc.at[entry].add(score * present)
        return ((grad_tok, score_acc), (gate_grad, up_grad, down_grad))
    start = (jnp.zeros((ntoken, D), jnp.float32), jnp.zeros((ntoken * TOP,), jnp.float32))
    (grad_tok, score_acc), (grad_gate, grad_up, grad_down) = lax.scan(expert_step, start, (table, present_all, gate_weight, up_weight, down_weight))
    score_tok = score_acc.reshape(ntoken, TOP)
    mixed = lax.optimization_barrier(jnp.sum(gates * score_tok, axis=1, keepdims=True))
    grad_chosen = gates * (score_tok - mixed)
    member = expert_ids[:, :, None] == labels
    grad_logits = lax.optimization_barrier(jnp.sum(jnp.where(member, grad_chosen[:, :, None], 0.0), axis=1)).astype(jnp.bfloat16)
    grad_normed = grad_tok + jnp.dot(grad_logits, router_weight.T, preferred_element_type=jnp.float32)
    grad_router = jnp.dot(normed.T, grad_logits, preferred_element_type=jnp.float32)
    grad_gain = lax.optimization_barrier(jnp.sum(grad_normed * scaled, axis=0))
    grad_scaled = grad_normed * norm_gain
    correction = lax.optimization_barrier(jnp.mean(grad_scaled * scaled, axis=1, keepdims=True))
    grad_tokens = (cotangent.astype(jnp.float32) + inverse * (grad_scaled - scaled * correction)).astype(jnp.bfloat16)
    return (grad_tokens, grad_gate, grad_up, grad_down, grad_router, grad_gain)
```

```python
import functools

import jax
import jax.numpy as jnp
from jax import lax
from jax.experimental import pallas as pl
from jax.experimental.pallas import tpu as pltpu
from jax.sharding import PartitionSpec as P

EPSILON = 1e-05
SWISH_SCALE = 1.702
LANES = 128
BF = jnp.bfloat16
F32 = jnp.float32


def dot(a, b, ca=1, cb=0):
    return lax.dot_general(a, b, (((ca,), (cb,)), ((), ())), preferred_element_type=F32)


def vmem(count):
    return [pl.BlockSpec(memory_space=pltpu.VMEM)] * count


def normalize(tokens_ref, gain_ref):
    widened = tokens_ref[...].astype(F32)
    inverse = lax.rsqrt(jnp.mean(widened * widened, axis=1, keepdims=True) + EPSILON)
    scaled = widened * inverse
    return inverse, scaled, (scaled * gain_ref[...]).astype(BF)


def slot_mask(table_t, first, local, cap, axis):
    rows = table_t.shape[1 - axis]
    shape = (local * cap, rows) if axis == 0 else (rows, local * cap)
    slot = lax.broadcasted_iota(jnp.int32, shape, axis)
    hit = None
    for e in range(local):
        line = table_t[first + e : first + e + 1, :] if axis == 0 else table_t[:, first + e : first + e + 1]
        one = line == (slot - e * cap).astype(F32)
        one = one & (slot >= e * cap) & (slot < (e + 1) * cap)
        hit = one if hit is None else hit | one
    return hit


def head_kernel(local, cap, tokens_ref, cot_ref, ids_ref, labels_ref, perm_ref, gain_ref, router_ref, *outs):
    messages, (rank_ref, gates_ref) = outs[:-2], outs[-2:]
    rows, width = tokens_ref.shape
    _, _, normed = normalize(tokens_ref, gain_ref)
    router = dot(router_ref[...], perm_ref[: router_ref.shape[1], :]).astype(BF)
    logits = dot(normed, router)
    member = None
    for k in range(ids_ref.shape[1]):
        one = ids_ref[:, k : k + 1] == labels_ref[...]
        member = one if member is None else member | one
    lifted = jnp.where(member, jnp.exp(jnp.where(member, logits, 0.0)), 0.0)
    gates = lifted / jnp.sum(lifted, axis=1, keepdims=True)
    upto = lax.broadcasted_iota(jnp.int32, (rows, rows), 0) >= lax.broadcasted_iota(jnp.int32, (rows, rows), 1)
    rank = dot(upto.astype(F32).astype(BF), member.astype(F32).astype(BF)) - 1.0
    rank = jnp.where(member, rank, -1.0)
    rank_ref[...] = rank
    gates_ref[...] = gates
    rank_t, gates_t = rank.T, gates.T
    cot = cot_ref[...]
    for s, out in enumerate(messages):
        hit = slot_mask(rank_t, s * local, local, cap, 0)
        slot = lax.broadcasted_iota(jnp.int32, hit.shape, 0)
        spread = None
        for e in range(local):
            line = gates_t[s * local + e : s * local + e + 1, :]
            part = jnp.where(hit & (slot >= e * cap) & (slot < (e + 1) * cap), line, 0.0)
            spread = part if spread is None else spread + part
        weight = jnp.sum(spread, axis=1, keepdims=True)
        pick = hit.astype(F32).astype(BF)
        out[:, :width] = dot(pick, normed).astype(BF)
        out[:, width:] = (dot(pick, cot) * weight).astype(BF)


def expert_kernel(width, near_ref, far_ref, gate_ref, up_ref, down_ref, *outs):
    gate, up, down = gate_ref[0], up_ref[0], down_ref[0]
    ff = gate.shape[1]
    for rows_ref, (back_ref, hidden_ref, pre_ref) in ((near_ref, outs[:3]), (far_ref, outs[3:])):
        rows = rows_ref[0, :, :width]
        gate_pre = dot(rows, gate)
        up_one = dot(rows, up) + 1.0
        grad = dot(rows_ref[0, :, width:], down, 1, 1)
        squash = jax.nn.sigmoid(SWISH_SCALE * gate_pre)
        swish = gate_pre * squash
        hidden = (swish * up_one).astype(BF)
        score = jnp.sum(grad * hidden.astype(F32), axis=1, keepdims=True)
        slope = squash + SWISH_SCALE * swish * (1.0 - squash)
        pre_gate = (grad * up_one * slope).astype(BF)
        pre_up = (grad * swish).astype(BF)
        hidden_ref[0] = hidden
        pre_ref[0, :, :ff] = pre_gate
        pre_ref[0, :, ff:] = pre_up
        back = dot(pre_gate, gate, 1, 1) + dot(pre_up, up, 1, 1)
        back_ref[0, :, :width] = back.astype(BF)
        lane = lax.broadcasted_iota(jnp.int32, (rows.shape[0], LANES), 1)
        back_ref[0, :, width:] = jnp.where(lane == 0, score, 0.0).astype(BF)


def weight_kernel(count, *refs):
    rows, ups = refs[:count], refs[count : 2 * count]
    hiddens, pres = refs[2 * count : 3 * count], refs[3 * count : 4 * count]
    gate_out, up_out, down_out = refs[4 * count :]
    ff = gate_out.shape[2]
    both = sum(dot(r[0], p[0], 0, 0) for r, p in zip(rows, pres))
    gate_out[0] = both[:, :ff].astype(BF)
    up_out[0] = both[:, ff:].astype(BF)
    down_out[0] = sum(dot(h[0], u[0], 0, 0) for h, u in zip(hiddens, ups)).astype(BF)


def tail_kernel(local, cap, experts, shard, count, *refs):
    pieces = refs[:count]
    rank_ref, gates_ref, tokens_ref, cot_ref, perm_ref, gain_ref, router_ref = refs[count : count + 7]
    grad_ref, part_ref, score_ref = refs[count + 7 :]
    width = tokens_ref.shape[1]
    rank, gates = rank_ref[...], gates_ref[...]
    rank_t = rank.T
    inverse, scaled, normed = normalize(tokens_ref, gain_ref)
    router = dot(router_ref[...], perm_ref[: router_ref.shape[1], :]).astype(BF)
    score_ref[...] = jnp.zeros(score_ref.shape, F32)
    back = None
    for s, piece in enumerate(pieces):
        pick = slot_mask(rank, s * local, local, cap, 1).astype(F32).astype(BF)
        part = dot(pick, piece[:, :width])
        back = part if back is None else back + part
        column = piece[:, width : width + LANES].astype(F32)[:, :1]
        hit = slot_mask(rank_t, s * local, local, cap, 0)
        slot = lax.broadcasted_iota(jnp.int32, hit.shape, 0)
        for e in range(local):
            mine = hit & (slot >= e * cap) & (slot < (e + 1) * cap)
            score_ref[s * local + e : s * local + e + 1, :] = jnp.sum(
                jnp.where(mine, column, 0.0), axis=0, keepdims=True
            )
    score = score_ref[...].T
    mixed = jnp.sum(score, axis=1, keepdims=True)
    grad_logits = jnp.where(rank >= 0.0, score - gates * mixed, 0.0).astype(BF)
    grad_normed = back + dot(grad_logits, router, 1, 1)
    natural = dot(grad_logits, perm_ref[...], 1, 1)
    part_t = dot(natural.T.astype(BF), normed)
    gain_part = jnp.sum(grad_normed * scaled, axis=0, keepdims=True)
    wide = part_ref.shape[1]
    line = lax.broadcasted_iota(jnp.int32, (wide, width), 0)
    part = jnp.where(line == experts, gain_part, part_t[:wide])
    part_ref[...] = jnp.zeros(part_ref.shape, F32)
    for d in range(part_ref.shape[0]):
        part_ref[d, :, :shard] = part[:, d * shard : (d + 1) * shard]
    grad_scaled = grad_normed * gain_ref[...]
    correction = jnp.mean(grad_scaled * scaled, axis=1, keepdims=True)
    grad_ref[...] = (
        cot_ref[...].astype(F32) + inverse * (grad_scaled - scaled * correction)
    ).astype(BF)


def after(value, *others):
    return lax.optimization_barrier((value, *others))[0]


def body(tokens, cotangent, expert_ids, norm_gain, router_weight, gate_weight, up_weight, down_weight):
    n_ctx, n_dp = lax.axis_size("ctx"), lax.axis_size("dp")
    me = lax.axis_index("ctx")
    local, width, ff = gate_weight.shape
    experts = router_weight.shape[1]
    rows_here, picks = expert_ids.shape
    cap = max(2, rows_here * picks * 5 // (4 * experts))
    slots = local * cap
    wide = width + LANES
    labels = jnp.arange(experts, dtype=jnp.int32)
    labels = ((labels // local) ^ me) * local + labels % local
    perm = (jnp.arange(LANES)[:, None] == labels[None, :]).astype(BF)
    perm = jnp.pad(perm, ((0, 0), (0, LANES - experts)))
    labels = jnp.pad(labels, (0, LANES - experts), constant_values=-1)[None, :]
    gain = norm_gain[None, :]
    limit = pltpu.CompilerParams(vmem_limit_bytes=56 * 1024 * 1024)

    *messages, rank, gates = pl.pallas_call(
        functools.partial(head_kernel, local, cap),
        out_shape=[jax.ShapeDtypeStruct((slots, 2 * width), BF)] * n_ctx
        + [jax.ShapeDtypeStruct((rows_here, LANES), F32)] * 2,
        in_specs=vmem(7),
        out_specs=vmem(n_ctx + 2),
        compiler_params=limit,
        name="head",
    )(tokens, cotangent, expert_ids, labels, perm, gain, router_weight)

    def across(value, s):
        return lax.ppermute(value, "ctx", [(i, i ^ s) for i in range(n_ctx)])

    def chip(value):
        return lax.ppermute(value, "dp", [(i, i ^ 2) for i in range(n_dp)])

    def core(value):
        return lax.ppermute(value, "dp", [(i, i ^ 1) for i in range(n_dp)])

    half, quarter = n_ctx // 2, n_ctx // 4
    groups = (range(half), range(half, half + quarter), range(half + quarter, n_ctx))
    arrived, crossed = {}, {}
    for s in range(n_ctx):
        value = messages[s]
        if s >= half + quarter:
            value = after(value, arrived[s - quarter])
        arrived[s] = across(value, s) if s else value
    for s in range(n_ctx):
        crossed[s] = chip(arrived[s])

    def expert_pass(near, far):
        rows = near.shape[1]
        spec = lambda *shape: pl.BlockSpec((1, *shape), lambda e: (e, 0, 0))
        outs = ((rows, wide), (rows, ff), (rows, 2 * ff)) * 2
        flops = 2 * 2 * local * rows * width * ff * 5
        return pl.pallas_call(
            functools.partial(expert_kernel, width),
            grid=(local,),
            in_specs=[spec(rows, 2 * width)] * 2 + [spec(width, ff)] * 2 + [spec(ff, width)],
            out_specs=[spec(*o) for o in outs],
            out_shape=[jax.ShapeDtypeStruct((local, *o), BF) for o in outs],
            compiler_params=limit,
            cost_estimate=pl.CostEstimate(flops=flops, bytes_accessed=16 * rows * width, transcendentals=0),
            name="expert",
        )(near, far, gate_weight, up_weight, down_weight)

    done = []
    for group in groups:
        parts = [arrived[s] for s in group] + [crossed[s] for s in group]
        near = jnp.concatenate([p.reshape(local, cap, 2 * width) for p in parts], axis=1)
        far = core(near)
        done.append((near, far, *expert_pass(near, far)))

    returned = {}
    for g in (1, 2, 0):
        group = groups[g]
        size = len(group) * cap
        back_near, back_far = done[g][2], done[g][5]
        other = core(back_far)
        leave = (back_near[:, size:].astype(F32) + other[:, size:].astype(F32)).astype(BF)
        came = chip(leave)
        for i, s in enumerate(group):
            cut = slice(i * cap, (i + 1) * cap)
            final = back_near[:, cut].astype(F32) + other[:, cut].astype(F32) + came[:, cut].astype(F32)
            final = final.astype(BF).reshape(slots, wide)
            returned[s] = across(final, s) if s else final

    near_rows = [d[0] for d in done] + [d[1] for d in done]
    hiddens = [d[3] for d in done] + [d[6] for d in done]
    pres = [d[4] for d in done] + [d[7] for d in done]
    count = len(near_rows)
    steps = 2
    tile = width // steps
    total = sum(r.shape[1] for r in near_rows)

    def weights():
        row_specs = [pl.BlockSpec((1, r.shape[1], tile), lambda e, j: (e, 0, j)) for r in near_rows]
        up_specs = [pl.BlockSpec((1, r.shape[1], tile), lambda e, j: (e, 0, j + steps)) for r in near_rows]
        hid_specs = [pl.BlockSpec((1, r.shape[1], ff), lambda e, j: (e, 0, 0)) for r in near_rows]
        pre_specs = [pl.BlockSpec((1, r.shape[1], 2 * ff), lambda e, j: (e, 0, 0)) for r in near_rows]
        return pl.pallas_call(
            functools.partial(weight_kernel, count),
            grid=(local, steps),
            in_specs=row_specs + up_specs + hid_specs + pre_specs,
            out_specs=[pl.BlockSpec((1, tile, ff), lambda e, j: (e, j, 0))] * 2
            + [pl.BlockSpec((1, ff, tile), lambda e, j: (e, 0, j))],
            out_shape=[jax.ShapeDtypeStruct((local, width, ff), BF)] * 2
            + [jax.ShapeDtypeStruct((local, ff, width), BF)],
            compiler_params=limit,
            cost_estimate=pl.CostEstimate(
                flops=2 * local * total * width * ff * 3, bytes_accessed=local * total * 4 * width, transcendentals=0
            ),
            name="weights",
        )(*near_rows, *near_rows, *hiddens, *pres)

    gate_grad, up_grad, down_grad = weights()

    devices = n_dp * n_ctx
    shard = width // devices
    lines = -(-(experts + 1) // 8) * 8
    grad_input, part = pl.pallas_call(
        functools.partial(tail_kernel, local, cap, experts, shard, n_ctx),
        out_shape=[
            jax.ShapeDtypeStruct((rows_here, width), BF),
            jax.ShapeDtypeStruct((devices, lines, LANES), F32),
        ],
        in_specs=vmem(n_ctx + 7),
        out_specs=vmem(2),
        scratch_shapes=[pltpu.VMEM((LANES, rows_here), F32)],
        compiler_params=limit,
        name="tail",
    )(*[returned[s] for s in range(n_ctx)], rank, gates, tokens, cotangent, perm, gain, router_weight)
    part = jnp.sum(lax.all_to_all(part, ("dp", "ctx"), 0, 0, tiled=True), axis=0)
    return (grad_input, gate_grad, up_grad, down_grad, part[:experts, :shard].T, part[experts, :shard])


def solution(mesh):
    return jax.shard_map(
        body,
        mesh=mesh,
        in_specs=(
            P(("dp", "ctx"), None),
            P(("dp", "ctx"), None),
            P(("dp", "ctx"), None),
            P(),
            P(),
            P("ctx", None, "dp"),
            P("ctx", None, "dp"),
            P("ctx", "dp", None),
        ),
        out_specs=(
            P(("dp", "ctx"), None),
            P("ctx", None, "dp"),
            P("ctx", None, "dp"),
            P("ctx", "dp", None),
            P(("dp", "ctx"), None),
            P(("dp", "ctx")),
        ),
        check_vma=False,
    )
```

```python
import functools

import jax
import jax.numpy as jnp
from jax import lax
from jax.experimental import pallas as pl
from jax.experimental.pallas import tpu as pltpu
from jax.sharding import PartitionSpec as P


EPSILON = 1e-05
SWISH_SCALE = 1.702
LANES = 128
BF = jnp.bfloat16
F32 = jnp.float32


def dot(a, b, ca=1, cb=0):
    return lax.dot_general(a, b, (((ca,), (cb,)), ((), ())), preferred_element_type=F32)


def vmem(count):
    return [pl.BlockSpec(memory_space=pltpu.VMEM)] * count


def normalize(tokens_ref, gain_ref):
    widened = tokens_ref[...].astype(F32)
    inverse = lax.rsqrt(jnp.mean(widened * widened, axis=1, keepdims=True) + EPSILON)
    scaled = widened * inverse
    gain = gain_ref[...][None, :]
    return inverse, scaled, (scaled * gain).astype(BF), gain


def permutation(labels_ref, count):
    shape = (labels_ref.shape[0], count)
    return (labels_ref[...] == lax.broadcasted_iota(jnp.int32, shape, 1)).astype(F32).astype(BF)


def slot_mask(table_t, first, local, cap, axis):
    rows = table_t.shape[1 - axis]
    shape = (local * cap, rows) if axis == 0 else (rows, local * cap)
    slot = lax.broadcasted_iota(jnp.int32, shape, axis)
    hit = None
    for e in range(local):
        line = table_t[first + e : first + e + 1, :] if axis == 0 else table_t[:, first + e : first + e + 1]
        one = line == (slot - e * cap).astype(F32)
        one = one & (slot >= e * cap) & (slot < (e + 1) * cap)
        hit = one if hit is None else hit | one
    return hit


def head_kernel(local, cap, tokens_ref, cot_ref, ids_ref, labels_ref, gain_ref, router_ref, *outs):
    messages, (rank_ref, gates_ref) = outs[:-2], outs[-2:]
    rows, width = tokens_ref.shape
    _, _, normed, _ = normalize(tokens_ref, gain_ref)
    router = dot(permutation(labels_ref, router_ref.shape[0]), router_ref[...]).astype(BF)
    logits = dot(router, normed, 1, 1)
    member = None
    for k in range(ids_ref.shape[0]):
        one = ids_ref[k : k + 1, :] == labels_ref[...]
        member = one if member is None else member | one
    lifted = jnp.where(member, jnp.exp(jnp.where(member, logits, 0.0)), 0.0)
    gates_t = lifted / jnp.sum(lifted, axis=0, keepdims=True)
    upto = lax.broadcasted_iota(jnp.int32, (rows, rows), 0) <= lax.broadcasted_iota(jnp.int32, (rows, rows), 1)
    rank_t = dot(member.astype(F32).astype(BF), upto.astype(F32).astype(BF)) - 1.0
    rank_t = jnp.where(member, rank_t, -1.0)
    rank_ref[...] = rank_t
    gates_ref[...] = gates_t
    cot = cot_ref[...]
    for s, out in enumerate(messages):
        hit = slot_mask(rank_t, s * local, local, cap, 0)
        slot = lax.broadcasted_iota(jnp.int32, hit.shape, 0)
        spread = None
        for e in range(local):
            line = gates_t[s * local + e : s * local + e + 1, :]
            part = jnp.where(hit & (slot >= e * cap) & (slot < (e + 1) * cap), line, 0.0)
            spread = part if spread is None else spread + part
        weight = jnp.sum(spread, axis=1, keepdims=True)
        pick = hit.astype(F32).astype(BF)
        out[:, :width] = dot(pick, normed).astype(BF)
        out[:, width:] = (dot(pick, cot) * weight).astype(BF)


def expert_kernel(width, near_ref, far_ref, gate_ref, up_ref, down_ref, *outs):
    gate, up, down = gate_ref[0], up_ref[0], down_ref[0]
    ff = gate.shape[1]
    for rows_ref, (back_ref, hidden_ref, pre_ref) in ((near_ref, outs[:3]), (far_ref, outs[3:])):
        rows = rows_ref[0, :, :width]
        gate_pre = dot(rows, gate)
        up_one = dot(rows, up) + 1.0
        grad = dot(rows_ref[0, :, width:], down, 1, 1)
        squash = jax.nn.sigmoid(SWISH_SCALE * gate_pre)
        swish = gate_pre * squash
        hidden = (swish * up_one).astype(BF)
        score = jnp.sum(grad * hidden.astype(F32), axis=1, keepdims=True)
        slope = squash + SWISH_SCALE * swish * (1.0 - squash)
        pre_gate = (grad * up_one * slope).astype(BF)
        pre_up = (grad * swish).astype(BF)
        hidden_ref[0] = hidden
        pre_ref[0, :, :ff] = pre_gate
        pre_ref[0, :, ff:] = pre_up
        back = dot(pre_gate, gate, 1, 1) + dot(pre_up, up, 1, 1)
        back_ref[0, :, :width] = back.astype(BF)
        lane = lax.broadcasted_iota(jnp.int32, (rows.shape[0], LANES), 1)
        back_ref[0, :, width:] = jnp.where(lane == 0, score, 0.0).astype(BF)


def weight_kernel(count, *refs):
    rows, ups = refs[:count], refs[count : 2 * count]
    hiddens, pres = refs[2 * count : 3 * count], refs[3 * count : 4 * count]
    gate_out, up_out, down_out = refs[-3:]
    ff = gate_out.shape[2]
    both = sum(dot(r[0], p[0], 0, 0) for r, p in zip(rows, pres))
    gate_out[0] = both[:, :ff].astype(BF)
    up_out[0] = both[:, ff:].astype(BF)
    down_out[0] = sum(dot(h[0], u[0], 0, 0) for h, u in zip(hiddens, ups)).astype(BF)


def tail_kernel(local, cap, experts, shard, count, *refs):
    pieces = refs[:count]
    rank_ref, gates_ref, tokens_ref, cot_ref, labels_ref, gain_ref, router_ref = refs[count : count + 7]
    grad_ref, part_ref, score_ref = refs[count + 7 :]
    width = tokens_ref.shape[1]
    rank_t = rank_ref[...]
    rank = rank_t.T
    inverse, scaled, normed, gain = normalize(tokens_ref, gain_ref)
    router = dot(permutation(labels_ref, experts), router_ref[...]).astype(BF)
    score_ref[...] = jnp.zeros(score_ref.shape, F32)
    back = None
    for s, piece in enumerate(pieces):
        pick = slot_mask(rank, s * local, local, cap, 1).astype(F32).astype(BF)
        part = dot(pick, piece[:, :width])
        back = part if back is None else back + part
        column = piece[:, width : width + LANES].astype(F32)[:, :1]
        hit = slot_mask(rank_t, s * local, local, cap, 0)
        slot = lax.broadcasted_iota(jnp.int32, hit.shape, 0)
        for e in range(local):
            mine = hit & (slot >= e * cap) & (slot < (e + 1) * cap)
            score_ref[s * local + e : s * local + e + 1, :] = jnp.sum(
                jnp.where(mine, column, 0.0), axis=0, keepdims=True
            )
    score = score_ref[...]
    mixed = jnp.sum(score, axis=0, keepdims=True)
    grad_logits = jnp.where(rank_t >= 0.0, score - gates_ref[...] * mixed, 0.0)
    grad_normed = back + dot(grad_logits.T.astype(BF), router)
    natural = dot(permutation(labels_ref, LANES), grad_logits.astype(BF), 0, 0)
    part_t = dot(natural.astype(BF), normed)
    gain_part = jnp.sum(grad_normed * scaled, axis=0, keepdims=True)
    wide = part_ref.shape[1]
    line = lax.broadcasted_iota(jnp.int32, (wide, width), 0)
    part = jnp.where(line == experts, gain_part, part_t[:wide])
    part_ref[...] = jnp.zeros(part_ref.shape, F32)
    for d in range(part_ref.shape[0]):
        part_ref[d, :, :shard] = part[:, d * shard : (d + 1) * shard]
    grad_scaled = grad_normed * gain
    correction = jnp.mean(grad_scaled * scaled, axis=1, keepdims=True)
    grad_ref[...] = (
        cot_ref[...].astype(F32) + inverse * (grad_scaled - scaled * correction)
    ).astype(BF)


def body(tokens, cotangent, expert_ids, norm_gain, router_weight, gate_weight, up_weight, down_weight):
    n_ctx, n_dp = lax.axis_size("ctx"), lax.axis_size("dp")
    me = lax.axis_index("ctx")
    local, width, ff = gate_weight.shape
    experts = router_weight.shape[1]
    rows_here, picks = expert_ids.shape
    cap = max(2, rows_here * picks * 5 // (4 * experts))
    slots = local * cap
    wide = width + LANES
    labels = jnp.arange(experts, dtype=jnp.int32)
    labels = ((labels // local) ^ me) * local + labels % local
    labels = jnp.pad(labels, (0, LANES - experts), constant_values=-1)[:, None]
    router = router_weight.T
    limit = pltpu.CompilerParams(vmem_limit_bytes=56 * 1024 * 1024)

    *messages, rank, gates = pl.pallas_call(
        functools.partial(head_kernel, local, cap),
        out_shape=[jax.ShapeDtypeStruct((slots, 2 * width), BF)] * n_ctx
        + [jax.ShapeDtypeStruct((rows_here, LANES), F32)] * 2,
        in_specs=vmem(6),
        out_specs=vmem(n_ctx + 2),
        compiler_params=limit,
        name="head",
    )(tokens, cotangent, expert_ids.T, labels, norm_gain, router)

    def across(value, s):
        return lax.ppermute(value, "ctx", [(i, i ^ s) for i in range(n_ctx)])

    def chip(value):
        return lax.ppermute(value, "dp", [(i, i ^ 2) for i in range(n_dp)])

    def core(value):
        return lax.ppermute(value, "dp", [(i, i ^ 1) for i in range(n_dp)])

    half, quarter = n_ctx // 2, n_ctx // 4
    groups = (range(half), range(half, half + quarter), range(half + quarter, n_ctx))
    arrived = {s: across(messages[s], s) if s else messages[s] for s in range(n_ctx)}
    crossed = {s: chip(arrived[s]) for s in range(n_ctx)}

    def expert_pass(near, far):
        rows = near.shape[1]
        spec = lambda *shape: pl.BlockSpec((1, *shape), lambda e: (e, 0, 0))
        outs = ((rows, wide), (rows, ff), (rows, 2 * ff)) * 2
        flops = 2 * 2 * local * rows * width * ff * 5
        return pl.pallas_call(
            functools.partial(expert_kernel, width),
            grid=(local,),
            in_specs=[spec(rows, 2 * width)] * 2 + [spec(width, ff)] * 2 + [spec(ff, width)],
            out_specs=[spec(*o) for o in outs],
            out_shape=[jax.ShapeDtypeStruct((local, *o), BF) for o in outs],
            compiler_params=limit,
            cost_estimate=pl.CostEstimate(flops=flops, bytes_accessed=16 * rows * width, transcendentals=0),
            name="expert",
        )(near, far, gate_weight, up_weight, down_weight)

    done = []
    for group in groups:
        parts = [arrived[s] for s in group] + [crossed[s] for s in group]
        near = jnp.concatenate([p.reshape(local, cap, 2 * width) for p in parts], axis=1)
        far = core(near)
        done.append((near, far, *expert_pass(near, far)))

    returned = {}
    for g in (1, 2, 0):
        group = groups[g]
        size = len(group) * cap
        back_near, back_far = done[g][2], done[g][5]
        other = core(back_far)
        leave = (back_near[:, size:].astype(F32) + other[:, size:].astype(F32)).astype(BF)
        came = chip(leave)
        for i, s in enumerate(group):
            cut = slice(i * cap, (i + 1) * cap)
            final = back_near[:, cut].astype(F32) + other[:, cut].astype(F32) + came[:, cut].astype(F32)
            final = final.astype(BF).reshape(slots, wide)
            returned[s] = across(final, s) if s else final

    near_rows = [d[0] for d in done] + [d[1] for d in done]
    hiddens = [d[3] for d in done] + [d[6] for d in done]
    pres = [d[4] for d in done] + [d[7] for d in done]
    count = len(near_rows)
    steps = 2
    tile = width // steps
    total = sum(r.shape[1] for r in near_rows)

    def weights(step):
        row_specs = [pl.BlockSpec((1, r.shape[1], tile), lambda e: (e, 0, step)) for r in near_rows]
        up_specs = [pl.BlockSpec((1, r.shape[1], tile), lambda e: (e, 0, step + steps)) for r in near_rows]
        hid_specs = [pl.BlockSpec((1, r.shape[1], ff), lambda e: (e, 0, 0)) for r in near_rows]
        pre_specs = [pl.BlockSpec((1, r.shape[1], 2 * ff), lambda e: (e, 0, 0)) for r in near_rows]
        carry = list(grads) if step else []
        return pl.pallas_call(
            functools.partial(weight_kernel, count),
            grid=(local,),
            in_specs=row_specs + up_specs + hid_specs + pre_specs + [pl.BlockSpec(memory_space=pl.ANY)] * len(carry),
            out_specs=[pl.BlockSpec((1, tile, ff), lambda e: (e, step, 0))] * 2
            + [pl.BlockSpec((1, ff, tile), lambda e: (e, 0, step))],
            out_shape=[jax.ShapeDtypeStruct((local, width, ff), BF)] * 2
            + [jax.ShapeDtypeStruct((local, ff, width), BF)],
            input_output_aliases={4 * count + i: i for i in range(len(carry))},
            compiler_params=limit,
            cost_estimate=pl.CostEstimate(
                flops=2 * local * total * tile * ff * 3, bytes_accessed=local * total * 4 * tile, transcendentals=0
            ),
        )(*near_rows, *near_rows, *hiddens, *pres, *carry)

    grads = None
    for step in range(steps):
        grads = weights(step)
    gate_grad, up_grad, down_grad = grads

    devices = n_dp * n_ctx
    shard = width // devices
    lines = -(-(experts + 1) // 8) * 8
    grad_input, part = pl.pallas_call(
        functools.partial(tail_kernel, local, cap, experts, shard, n_ctx),
        out_shape=[
            jax.ShapeDtypeStruct((rows_here, width), BF),
            jax.ShapeDtypeStruct((devices, lines, LANES), F32),
        ],
        in_specs=vmem(n_ctx + 7),
        out_specs=vmem(2),
        scratch_shapes=[pltpu.VMEM((LANES, rows_here), F32)],
        compiler_params=limit,
        name="tail",
    )(*[returned[s] for s in range(n_ctx)], rank, gates, tokens, cotangent, labels, norm_gain, router)
    part = jnp.sum(lax.all_to_all(part, ("dp", "ctx"), 0, 0, tiled=True), axis=0)
    return (grad_input, gate_grad, up_grad, down_grad, part[:experts, :shard].T, part[experts, :shard])


def solution(mesh):
    return jax.shard_map(
        body,
        mesh=mesh,
        in_specs=(
            P(("dp", "ctx"), None),
            P(("dp", "ctx"), None),
            P(("dp", "ctx"), None),
            P(),
            P(),
            P("ctx", None, "dp"),
            P("ctx", None, "dp"),
            P("ctx", "dp", None),
        ),
        out_specs=(
            P(("dp", "ctx"), None),
            P("ctx", None, "dp"),
            P("ctx", None, "dp"),
            P("ctx", "dp", None),
            P(("dp", "ctx"), None),
            P(("dp", "ctx")),
        ),
        check_vma=False,
    )
```

```python
import functools

import jax
import jax.numpy as jnp
from jax import lax
from jax.experimental import pallas as pl
from jax.experimental.pallas import tpu as pltpu
from jax.sharding import PartitionSpec as P


EPSILON = 1e-05
SWISH_SCALE = 1.702
LANES = 128
BF = jnp.bfloat16
F32 = jnp.float32


def dot(a, b, ca=1, cb=0):
    return lax.dot_general(a, b, (((ca,), (cb,)), ((), ())), preferred_element_type=F32)


def vmem(count):
    return [pl.BlockSpec(memory_space=pltpu.VMEM)] * count


def normalize(tokens_ref, gain_ref):
    widened = tokens_ref[...].astype(F32)
    inverse = lax.rsqrt(jnp.mean(widened * widened, axis=1, keepdims=True) + EPSILON)
    scaled = widened * inverse
    gain = gain_ref[...][None, :]
    return inverse, scaled, (scaled * gain).astype(BF), gain


def permutation(labels_ref, count):
    shape = (labels_ref.shape[0], count)
    return (labels_ref[...] == lax.broadcasted_iota(jnp.int32, shape, 1)).astype(F32).astype(BF)


def slot_mask(table_t, first, local, cap, axis):
    rows = table_t.shape[1 - axis]
    shape = (local * cap, rows) if axis == 0 else (rows, local * cap)
    slot = lax.broadcasted_iota(jnp.int32, shape, axis)
    hit = None
    for e in range(local):
        line = table_t[first + e : first + e + 1, :] if axis == 0 else table_t[:, first + e : first + e + 1]
        one = line == (slot - e * cap).astype(F32)
        one = one & (slot >= e * cap) & (slot < (e + 1) * cap)
        hit = one if hit is None else hit | one
    return hit


def head_kernel(local, cap, tokens_ref, cot_ref, ids_ref, labels_ref, gain_ref, router_ref, *outs):
    messages, (rank_ref, gates_ref) = outs[:-2], outs[-2:]
    rows, width = tokens_ref.shape
    _, _, normed, _ = normalize(tokens_ref, gain_ref)
    router = dot(permutation(labels_ref, router_ref.shape[0]), router_ref[...]).astype(BF)
    logits = dot(router, normed, 1, 1)
    member = None
    for k in range(ids_ref.shape[0]):
        one = ids_ref[k : k + 1, :] == labels_ref[...]
        member = one if member is None else member | one
    lifted = jnp.where(member, jnp.exp(jnp.where(member, logits, 0.0)), 0.0)
    gates_t = lifted / jnp.sum(lifted, axis=0, keepdims=True)
    upto = lax.broadcasted_iota(jnp.int32, (rows, rows), 0) <= lax.broadcasted_iota(jnp.int32, (rows, rows), 1)
    rank_t = dot(member.astype(F32).astype(BF), upto.astype(F32).astype(BF)) - 1.0
    rank_t = jnp.where(member, rank_t, -1.0)
    rank_ref[...] = rank_t
    gates_ref[...] = gates_t
    cot = cot_ref[...]
    for s, out in enumerate(messages):
        hit = slot_mask(rank_t, s * local, local, cap, 0)
        slot = lax.broadcasted_iota(jnp.int32, hit.shape, 0)
        spread = None
        for e in range(local):
            line = gates_t[s * local + e : s * local + e + 1, :]
            part = jnp.where(hit & (slot >= e * cap) & (slot < (e + 1) * cap), line, 0.0)
            spread = part if spread is None else spread + part
        weight = jnp.sum(spread, axis=1, keepdims=True)
        pick = hit.astype(F32).astype(BF)
        out[:, :width] = dot(pick, normed).astype(BF)
        out[:, width:] = (dot(pick, cot) * weight).astype(BF)


def expert_kernel(width, near_ref, far_ref, gate_ref, up_ref, down_ref, *outs):
    gate, up, down = gate_ref[0], up_ref[0], down_ref[0]
    ff = gate.shape[1]
    for rows_ref, (back_ref, hidden_ref, pre_ref) in ((near_ref, outs[:3]), (far_ref, outs[3:])):
        rows = rows_ref[0, :, :width]
        gate_pre = dot(rows, gate)
        up_one = dot(rows, up) + 1.0
        grad = dot(rows_ref[0, :, width:], down, 1, 1)
        squash = jax.nn.sigmoid(SWISH_SCALE * gate_pre)
        swish = gate_pre * squash
        hidden = (swish * up_one).astype(BF)
        score = jnp.sum(grad * hidden.astype(F32), axis=1, keepdims=True)
        slope = squash + SWISH_SCALE * swish * (1.0 - squash)
        pre_gate = (grad * up_one * slope).astype(BF)
        pre_up = (grad * swish).astype(BF)
        hidden_ref[0] = hidden
        pre_ref[0, :, :ff] = pre_gate
        pre_ref[0, :, ff:] = pre_up
        back = dot(pre_gate, gate, 1, 1) + dot(pre_up, up, 1, 1)
        back_ref[0, :, :width] = back.astype(BF)
        lane = lax.broadcasted_iota(jnp.int32, (rows.shape[0], LANES), 1)
        back_ref[0, :, width:] = jnp.where(lane == 0, score, 0.0).astype(BF)


def weight_kernel(count, *refs):
    rows, ups = refs[:count], refs[count : 2 * count]
    hiddens, pres = refs[2 * count : 3 * count], refs[3 * count : 4 * count]
    gate_out, up_out, down_out = refs[-3:]
    ff = gate_out.shape[2]
    both = sum(dot(r[0], p[0], 0, 0) for r, p in zip(rows, pres))
    gate_out[0] = both[:, :ff].astype(BF)
    up_out[0] = both[:, ff:].astype(BF)
    down_out[0] = sum(dot(h[0], u[0], 0, 0) for h, u in zip(hiddens, ups)).astype(BF)


def tail_kernel(local, cap, experts, shard, count, *refs):
    pieces = refs[:count]
    rank_ref, gates_ref, tokens_ref, cot_ref, labels_ref, gain_ref, router_ref = refs[count : count + 7]
    grad_ref, part_ref, score_ref = refs[count + 7 :]
    width = tokens_ref.shape[1]
    rank_t = rank_ref[...]
    rank = rank_t.T
    inverse, scaled, normed, gain = normalize(tokens_ref, gain_ref)
    router = dot(permutation(labels_ref, experts), router_ref[...]).astype(BF)
    score_ref[...] = jnp.zeros(score_ref.shape, F32)
    back = None
    for s, piece in enumerate(pieces):
        pick = slot_mask(rank, s * local, local, cap, 1).astype(F32).astype(BF)
        part = dot(pick, piece[:, :width])
        back = part if back is None else back + part
        column = piece[:, width : width + LANES].astype(F32)[:, :1]
        hit = slot_mask(rank_t, s * local, local, cap, 0)
        slot = lax.broadcasted_iota(jnp.int32, hit.shape, 0)
        for e in range(local):
            mine = hit & (slot >= e * cap) & (slot < (e + 1) * cap)
            score_ref[s * local + e : s * local + e + 1, :] = jnp.sum(
                jnp.where(mine, column, 0.0), axis=0, keepdims=True
            )
    score = score_ref[...]
    mixed = jnp.sum(score, axis=0, keepdims=True)
    grad_logits = jnp.where(rank_t >= 0.0, score - gates_ref[...] * mixed, 0.0)
    grad_normed = back + dot(grad_logits.T.astype(BF), router)
    natural = dot(permutation(labels_ref, LANES), grad_logits.astype(BF), 0, 0)
    part_t = dot(natural.astype(BF), normed)
    gain_part = jnp.sum(grad_normed * scaled, axis=0, keepdims=True)
    wide = part_ref.shape[1]
    line = lax.broadcasted_iota(jnp.int32, (wide, width), 0)
    part = jnp.where(line == experts, gain_part, part_t[:wide])
    part_ref[...] = jnp.zeros(part_ref.shape, F32)
    for d in range(part_ref.shape[0]):
        part_ref[d, :, :shard] = part[:, d * shard : (d + 1) * shard]
    grad_scaled = grad_normed * gain
    correction = jnp.mean(grad_scaled * scaled, axis=1, keepdims=True)
    grad_ref[...] = (
        cot_ref[...].astype(F32) + inverse * (grad_scaled - scaled * correction)
    ).astype(BF)


def add_kernel(*refs):
    total = refs[0][...].astype(F32)
    for ref in refs[1:-1]:
        total = total + ref[...].astype(F32)
    refs[-1][...] = total.astype(BF)


def add_pieces(*terms, count):
    local, _, cap, wide = terms[0][0].shape
    block = (local, 1, cap, wide)
    return pl.pallas_call(
        add_kernel,
        grid=(count,),
        in_specs=[pl.BlockSpec(block, lambda i, at=at: (0, at + i, 0, 0)) for _, at in terms],
        out_specs=pl.BlockSpec(block, lambda i: (0, i, 0, 0)),
        out_shape=jax.ShapeDtypeStruct((local, count, cap, wide), BF),
        name="add",
    )(*[value for value, _ in terms])


def plan(n_ctx):
    if n_ctx == 8:
        return ((0, 1, 2, 4), (3, 5), (6, 7)), (((4,), (0,), (1, 2)), ((5,), (3,)), ((6,), (7,)))
    half, quarter = n_ctx // 2, n_ctx // 4
    groups = (tuple(range(half)), tuple(range(half, half + quarter)), tuple(range(half + quarter, n_ctx)))
    return groups, tuple((g,) for g in groups)


def body(tokens, cotangent, expert_ids, norm_gain, router_weight, gate_weight, up_weight, down_weight):
    n_ctx, n_dp = lax.axis_size("ctx"), lax.axis_size("dp")
    me = lax.axis_index("ctx")
    local, width, ff = gate_weight.shape
    experts = router_weight.shape[1]
    rows_here, picks = expert_ids.shape
    cap = max(2, rows_here * picks * 5 // (4 * experts))
    slots = local * cap
    wide = width + LANES
    labels = jnp.arange(experts, dtype=jnp.int32)
    labels = ((labels // local) ^ me) * local + labels % local
    labels = jnp.pad(labels, (0, LANES - experts), constant_values=-1)[:, None]
    router = router_weight.T
    limit = pltpu.CompilerParams(vmem_limit_bytes=56 * 1024 * 1024)

    *messages, rank, gates = pl.pallas_call(
        functools.partial(head_kernel, local, cap),
        out_shape=[jax.ShapeDtypeStruct((slots, 2 * width), BF)] * n_ctx
        + [jax.ShapeDtypeStruct((rows_here, LANES), F32)] * 2,
        in_specs=vmem(6),
        out_specs=vmem(n_ctx + 2),
        compiler_params=limit,
        name="head",
    )(tokens, cotangent, expert_ids.T, labels, norm_gain, router)

    def across(value, s):
        return lax.ppermute(value, "ctx", [(i, i ^ s) for i in range(n_ctx)])

    def chip(value):
        return lax.ppermute(value, "dp", [(i, i ^ 2) for i in range(n_dp)])

    def core(value):
        return lax.ppermute(value, "dp", [(i, i ^ 1) for i in range(n_dp)])

    groups, units = plan(n_ctx)
    arrived = {s: across(messages[s], s) if s else messages[s] for s in range(n_ctx)}
    crossed = {s: chip(arrived[s]) for s in range(n_ctx)}

    def expert_pass(near, far):
        rows = near.shape[1]
        spec = lambda *shape: pl.BlockSpec((1, *shape), lambda e: (e, 0, 0))
        outs = ((rows, wide), (rows, ff), (rows, 2 * ff)) * 2
        flops = 2 * 2 * local * rows * width * ff * 5
        return pl.pallas_call(
            functools.partial(expert_kernel, width),
            grid=(local,),
            in_specs=[spec(rows, 2 * width)] * 2 + [spec(width, ff)] * 2 + [spec(ff, width)],
            out_specs=[spec(*o) for o in outs],
            out_shape=[jax.ShapeDtypeStruct((local, *o), BF) for o in outs],
            compiler_params=limit,
            cost_estimate=pl.CostEstimate(flops=flops, bytes_accessed=16 * rows * width, transcendentals=0),
            name="expert",
        )(near, far, gate_weight, up_weight, down_weight)

    done = []
    for group in groups:
        parts = lax.optimization_barrier([arrived[s] for s in group] + [crossed[s] for s in group])
        near = jnp.concatenate([p.reshape(local, cap, 2 * width) for p in parts], axis=1)
        far = core(near)
        done.append((near, far, *expert_pass(near, far)))

    returned = {}
    for g, group in enumerate(groups):
        split = lambda v: v.reshape(local, 2 * len(group), cap, wide)
        near, other = split(done[g][2]), split(core(done[g][5]))
        for unit in units[g]:
            first, size = group.index(unit[0]), len(unit)
            leave = add_pieces((near, len(group) + first), (other, len(group) + first), count=size)
            came = chip(leave)
            for i, s in enumerate(unit):
                final = add_pieces((near, first + i), (other, first + i), (came, i), count=1)
                final = final.reshape(slots, wide)
                returned[s] = across(final, s) if s else final

    near_rows = [d[0] for d in done] + [d[1] for d in done]
    hiddens = [d[3] for d in done] + [d[6] for d in done]
    pres = [d[4] for d in done] + [d[7] for d in done]
    count = len(near_rows)
    steps = 2
    tile = width // steps
    total = sum(r.shape[1] for r in near_rows)

    def weights(step):
        row_specs = [pl.BlockSpec((1, r.shape[1], tile), lambda e: (e, 0, step)) for r in near_rows]
        up_specs = [pl.BlockSpec((1, r.shape[1], tile), lambda e: (e, 0, step + steps)) for r in near_rows]
        hid_specs = [pl.BlockSpec((1, r.shape[1], ff), lambda e: (e, 0, 0)) for r in near_rows]
        pre_specs = [pl.BlockSpec((1, r.shape[1], 2 * ff), lambda e: (e, 0, 0)) for r in near_rows]
        carry = list(grads) if step else []
        return pl.pallas_call(
            functools.partial(weight_kernel, count),
            grid=(local,),
            in_specs=row_specs + up_specs + hid_specs + pre_specs + [pl.BlockSpec(memory_space=pl.ANY)] * len(carry),
            out_specs=[pl.BlockSpec((1, tile, ff), lambda e: (e, step, 0))] * 2
            + [pl.BlockSpec((1, ff, tile), lambda e: (e, 0, step))],
            out_shape=[jax.ShapeDtypeStruct((local, width, ff), BF)] * 2
            + [jax.ShapeDtypeStruct((local, ff, width), BF)],
            input_output_aliases={4 * count + i: i for i in range(len(carry))},
            compiler_params=limit,
            cost_estimate=pl.CostEstimate(
                flops=2 * local * total * tile * ff * 3, bytes_accessed=local * total * 4 * tile, transcendentals=0
            ),
        )(*near_rows, *near_rows, *hiddens, *pres, *carry)

    grads = None
    for step in range(steps):
        grads = weights(step)
    gate_grad, up_grad, down_grad = grads

    devices = n_dp * n_ctx
    shard = width // devices
    lines = -(-(experts + 1) // 8) * 8
    grad_input, part = pl.pallas_call(
        functools.partial(tail_kernel, local, cap, experts, shard, n_ctx),
        out_shape=[jax.ShapeDtypeStruct((rows_here, width), BF), jax.ShapeDtypeStruct((devices, lines, LANES), F32)],
        in_specs=vmem(n_ctx + 7),
        out_specs=vmem(2),
        scratch_shapes=[pltpu.VMEM((LANES, rows_here), F32)],
        compiler_params=limit,
        name="tail",
    )(*[returned[s] for s in range(n_ctx)], rank, gates, tokens, cotangent, labels, norm_gain, router)
    part = jnp.sum(lax.all_to_all(part, ("dp", "ctx"), 0, 0, tiled=True), axis=0)
    return (grad_input, gate_grad, up_grad, down_grad, part[:experts, :shard].T, part[experts, :shard])


def solution(mesh):
    return jax.shard_map(
        body,
        mesh=mesh,
        in_specs=(
            P(("dp", "ctx"), None),
            P(("dp", "ctx"), None),
            P(("dp", "ctx"), None),
            P(),
            P(),
            P("ctx", None, "dp"),
            P("ctx", None, "dp"),
            P("ctx", "dp", None),
        ),
        out_specs=(
            P(("dp", "ctx"), None),
            P("ctx", None, "dp"),
            P("ctx", None, "dp"),
            P("ctx", "dp", None),
            P(("dp", "ctx"), None),
            P(("dp", "ctx")),
        ),
        check_vma=False,
    )
```

```python
import functools

import jax
import jax.numpy as jnp
from jax import lax
from jax.experimental import pallas as pl
from jax.experimental.pallas import tpu as pltpu
from jax.sharding import PartitionSpec as P


EPSILON = 1e-05
SWISH_SCALE = 1.702
LANES = 128
BF = jnp.bfloat16
F32 = jnp.float32


def dot(a, b, ca=1, cb=0):
    return lax.dot_general(a, b, (((ca,), (cb,)), ((), ())), preferred_element_type=F32)


def vmem(count):
    return [pl.BlockSpec(memory_space=pltpu.VMEM)] * count


def normalize(tokens_ref, gain_ref):
    widened = tokens_ref[...].astype(F32)
    inverse = lax.rsqrt(jnp.mean(widened * widened, axis=1, keepdims=True) + EPSILON)
    scaled = widened * inverse
    gain = gain_ref[...][None, :]
    return inverse, scaled, (scaled * gain).astype(BF), gain


def permutation(labels_ref, count):
    shape = (labels_ref.shape[0], count)
    return (labels_ref[...] == lax.broadcasted_iota(jnp.int32, shape, 1)).astype(F32).astype(BF)


def slot_mask(table_t, first, local, cap, axis):
    rows = table_t.shape[1 - axis]
    shape = (local * cap, rows) if axis == 0 else (rows, local * cap)
    slot = lax.broadcasted_iota(jnp.int32, shape, axis)
    hit = None
    for e in range(local):
        line = table_t[first + e : first + e + 1, :] if axis == 0 else table_t[:, first + e : first + e + 1]
        one = line == (slot - e * cap).astype(F32)
        one = one & (slot >= e * cap) & (slot < (e + 1) * cap)
        hit = one if hit is None else hit | one
    return hit


def head_kernel(local, cap, tokens_ref, cot_ref, ids_ref, labels_ref, gain_ref, router_ref, *outs):
    messages, (rank_ref, gates_ref) = outs[:-2], outs[-2:]
    rows, width = tokens_ref.shape
    _, _, normed, _ = normalize(tokens_ref, gain_ref)
    router = dot(permutation(labels_ref, router_ref.shape[0]), router_ref[...]).astype(BF)
    logits = dot(router, normed, 1, 1)
    member = None
    for k in range(ids_ref.shape[0]):
        one = ids_ref[k : k + 1, :] == labels_ref[...]
        member = one if member is None else member | one
    lifted = jnp.where(member, jnp.exp(jnp.where(member, logits, 0.0)), 0.0)
    gates_t = lifted / jnp.sum(lifted, axis=0, keepdims=True)
    upto = lax.broadcasted_iota(jnp.int32, (rows, rows), 0) <= lax.broadcasted_iota(jnp.int32, (rows, rows), 1)
    rank_t = dot(member.astype(F32).astype(BF), upto.astype(F32).astype(BF)) - 1.0
    rank_t = jnp.where(member, rank_t, -1.0)
    rank_ref[...] = rank_t
    gates_ref[...] = gates_t
    cot = cot_ref[...]
    for s, out in enumerate(messages):
        hit = slot_mask(rank_t, s * local, local, cap, 0)
        slot = lax.broadcasted_iota(jnp.int32, hit.shape, 0)
        spread = None
        for e in range(local):
            line = gates_t[s * local + e : s * local + e + 1, :]
            part = jnp.where(hit & (slot >= e * cap) & (slot < (e + 1) * cap), line, 0.0)
            spread = part if spread is None else spread + part
        weight = jnp.sum(spread, axis=1, keepdims=True)
        pick = hit.astype(F32).astype(BF)
        out[:, :width] = dot(pick, normed).astype(BF)
        out[:, width:] = (dot(pick, cot) * weight).astype(BF)


def prepare_kernel(gate_ref, up_ref, down_ref, both_ref, turned_ref, down_out):
    ff = gate_ref.shape[2]
    both_ref[0, :, :ff] = gate_ref[0]
    both_ref[0, :, ff:] = up_ref[0]
    turned_ref[0, :ff, :] = gate_ref[0].T
    turned_ref[0, ff:, :] = up_ref[0].T
    down_out[0] = down_ref[0].T


def expert_kernel(width, near_ref, far_ref, both_ref, turned_ref, down_ref, *outs):
    both, turned, down = both_ref[0], turned_ref[0], down_ref[0]
    ff = down.shape[1]
    for rows_ref, (back_ref, hidden_ref, pre_ref) in ((near_ref, outs[:3]), (far_ref, outs[3:])):
        pre = dot(rows_ref[0, :, :width], both)
        gate_pre, up_one = pre[:, :ff], pre[:, ff:] + 1.0
        grad = dot(rows_ref[0, :, width:], down)
        squash = jax.nn.sigmoid(SWISH_SCALE * gate_pre)
        swish = gate_pre * squash
        hidden = (swish * up_one).astype(BF)
        score = jnp.sum(grad * hidden.astype(F32), axis=1, keepdims=True)
        slope = squash + SWISH_SCALE * swish * (1.0 - squash)
        hidden_ref[0] = hidden
        pre_ref[0, :, :ff] = (grad * up_one * slope).astype(BF)
        pre_ref[0, :, ff:] = (grad * swish).astype(BF)
        back_ref[0, :, :width] = dot(pre_ref[0], turned).astype(BF)
        lane = lax.broadcasted_iota(jnp.int32, (score.shape[0], LANES), 1)
        back_ref[0, :, width:] = jnp.where(lane == 0, score, 0.0).astype(BF)


def weight_kernel(count, *refs):
    gate_out, up_out, down_out, rows_ref, ups_ref, hid_ref, pre_ref = refs[-7:]
    ff = gate_out.shape[2]
    for n, joined in enumerate((rows_ref, ups_ref, hid_ref, pre_ref)):
        at = 0
        for piece in refs[n * count : (n + 1) * count]:
            joined[at : at + piece.shape[1]] = piece[0]
            at += piece.shape[1]
    both = dot(rows_ref[...], pre_ref[...], 0, 0)
    gate_out[0] = both[:, :ff].astype(BF)
    up_out[0] = both[:, ff:].astype(BF)
    down_out[0] = dot(hid_ref[...], ups_ref[...], 0, 0).astype(BF)


def tail_kernel(local, cap, experts, shard, packed, sources, *refs):
    count = len(sources)
    pieces = refs[:count]
    rank_ref, gates_ref, tokens_ref, cot_ref, labels_ref, gain_ref, router_ref = refs[count : count + 7]
    grad_ref, part_ref, score_ref = refs[count + 7 :]
    width = tokens_ref.shape[1]
    rank_t = rank_ref[...]
    rank = rank_t.T
    inverse, scaled, normed, gain = normalize(tokens_ref, gain_ref)
    router = dot(permutation(labels_ref, experts), router_ref[...]).astype(BF)
    score_ref[...] = jnp.zeros(score_ref.shape, F32)
    back = None
    for s, piece in zip(sources, pieces):
        pick = slot_mask(rank, s * local, local, cap, 1).astype(F32).astype(BF)
        part = dot(pick, piece[:, :width])
        back = part if back is None else back + part
        column = piece[:, width : width + LANES].astype(F32)[:, :1]
        hit = slot_mask(rank_t, s * local, local, cap, 0)
        slot = lax.broadcasted_iota(jnp.int32, hit.shape, 0)
        for e in range(local):
            mine = hit & (slot >= e * cap) & (slot < (e + 1) * cap)
            score_ref[s * local + e : s * local + e + 1, :] += jnp.sum(
                jnp.where(mine, column, 0.0), axis=0, keepdims=True
            )
    score = score_ref[...]
    mixed = jnp.sum(score, axis=0, keepdims=True)
    grad_logits = jnp.where(rank_t >= 0.0, score - gates_ref[...] * mixed, 0.0)
    grad_normed = back + dot(grad_logits.T.astype(BF), router)
    natural = dot(permutation(labels_ref, LANES), grad_logits.astype(BF), 0, 0)
    part_t = dot(natural.astype(BF), normed)
    gain_part = jnp.sum(grad_normed * scaled, axis=0, keepdims=True)
    line = lax.broadcasted_iota(jnp.int32, (LANES, width), 0)
    part = jnp.where(line == experts, gain_part, part_t)
    if packed:
        columns = part.T
        for d in range(part_ref.shape[0]):
            first = d * shard
            total = columns[first : first + 8]
            for g in range(1, shard // 8):
                total = total + pltpu.roll(columns[first + 8 * g : first + 8 * g + 8], g * (experts + 1), 1)
            part_ref[d] = total
    else:
        part_ref[...] = jnp.zeros(part_ref.shape, F32)
        for d in range(part_ref.shape[0]):
            part_ref[d, :, :shard] = part[: part_ref.shape[1], d * shard : (d + 1) * shard]
    grad_scaled = grad_normed * gain
    correction = jnp.mean(grad_scaled * scaled, axis=1, keepdims=True)
    grad_ref[...] = (
        cot_ref[...].astype(F32) + inverse * (grad_scaled - scaled * correction)
    ).astype(BF)


def sum_kernel(sizes, near_ref, other_ref, *outs):
    count = sum(sizes)
    at = 0
    for size, leave, own in zip(sizes, outs[: len(sizes)], outs[len(sizes) :]):
        for out, first in ((leave, count + at), (own, at)):
            cut = slice(first, first + size)
            out[0] = (near_ref[0, cut].astype(F32) + other_ref[0, cut].astype(F32)).astype(BF)
        at += size


def sum_group(near, other, sizes):
    local, count, cap, wide = near.shape
    spec = lambda size: pl.BlockSpec((1, size, cap, wide), lambda e: (e, 0, 0, 0))
    outs = pl.pallas_call(
        functools.partial(sum_kernel, sizes),
        grid=(local,),
        in_specs=[spec(count)] * 2,
        out_specs=[spec(size) for size in sizes] * 2,
        out_shape=[jax.ShapeDtypeStruct((local, size, cap, wide), BF) for size in sizes] * 2,
        name="sum",
    )(near, other)
    return outs[: len(sizes)], outs[len(sizes) :]


def finish_kernel(experts, in_ref, router_ref, gain_ref):
    total = jnp.sum(in_ref[...], axis=0)
    turned = jnp.concatenate([total] * (LANES // 8), axis=0).T
    for g in range(router_ref.shape[0] // 8):
        block = pltpu.roll(total, -g * (experts + 1) % LANES, 1) if g else total
        router_ref[8 * g : 8 * g + 8, :] = block[:, :experts]
        line = g * (experts + 1) + experts
        gain_ref[:, 8 * g : 8 * g + 8] = turned[line : line + 1, 8 * g : 8 * g + 8]


def plan(n_ctx):
    if n_ctx == 8:
        return ((0, 1, 2, 4), (3, 5), (6, 7)), (((0,), (1, 2), (4,)), ((3,), (5,)), ((6,), (7,)))
    half, quarter = n_ctx // 2, n_ctx // 4
    groups = (tuple(range(half)), tuple(range(half, half + quarter)), tuple(range(half + quarter, n_ctx)))
    return groups, tuple((g,) for g in groups)


def body(tokens, cotangent, expert_ids, norm_gain, router_weight, gate_weight, up_weight, down_weight):
    n_ctx, n_dp = lax.axis_size("ctx"), lax.axis_size("dp")
    me = lax.axis_index("ctx")
    local, width, ff = gate_weight.shape
    experts = router_weight.shape[1]
    rows_here, picks = expert_ids.shape
    cap = max(2, rows_here * picks * 5 // (4 * experts))
    slots = local * cap
    wide = width + LANES
    labels = jnp.arange(experts, dtype=jnp.int32)
    labels = ((labels // local) ^ me) * local + labels % local
    labels = jnp.pad(labels, (0, LANES - experts), constant_values=-1)[:, None]
    router = router_weight.T
    limit = pltpu.CompilerParams(vmem_limit_bytes=56 * 1024 * 1024)

    *messages, rank, gates = pl.pallas_call(
        functools.partial(head_kernel, local, cap),
        out_shape=[jax.ShapeDtypeStruct((slots, 2 * width), BF)] * n_ctx
        + [jax.ShapeDtypeStruct((rows_here, LANES), F32)] * 2,
        in_specs=vmem(6),
        out_specs=vmem(n_ctx + 2),
        compiler_params=limit,
        name="head",
    )(tokens, cotangent, expert_ids.T, labels, norm_gain, router)

    def across(value, s):
        return lax.ppermute(value, "ctx", [(i, i ^ s) for i in range(n_ctx)])

    def chip(value):
        return lax.ppermute(value, "dp", [(i, i ^ 2) for i in range(n_dp)])

    def core(value):
        return lax.ppermute(value, "dp", [(i, i ^ 1) for i in range(n_dp)])

    groups, units = plan(n_ctx)
    arrived = {s: across(messages[s], s) if s else messages[s] for s in range(n_ctx)}
    crossed = {s: chip(arrived[s]) for s in range(n_ctx)}

    turn = lambda *shape: pl.BlockSpec((1, *shape), lambda e: (e, 0, 0))
    turned_shapes = ((width, 2 * ff), (2 * ff, width), (width, ff))
    prepared = pl.pallas_call(
        prepare_kernel,
        grid=(local,),
        in_specs=[turn(width, ff)] * 2 + [turn(ff, width)],
        out_specs=[turn(*t) for t in turned_shapes],
        out_shape=[jax.ShapeDtypeStruct((local, *t), BF) for t in turned_shapes],
        compiler_params=limit,
        name="prepare",
    )(gate_weight, up_weight, down_weight)

    def expert_pass(near, far):
        rows = near.shape[1]
        spec = lambda *shape: pl.BlockSpec((1, *shape), lambda e: (e, 0, 0))
        outs = ((rows, wide), (rows, ff), (rows, 2 * ff)) * 2
        flops = 2 * 2 * local * rows * width * ff * 5
        return pl.pallas_call(
            functools.partial(expert_kernel, width),
            grid=(local,),
            in_specs=[spec(rows, 2 * width)] * 2 + [spec(width, 2 * ff), spec(2 * ff, width), spec(width, ff)],
            out_specs=[spec(*o) for o in outs],
            out_shape=[jax.ShapeDtypeStruct((local, *o), BF) for o in outs],
            compiler_params=limit,
            cost_estimate=pl.CostEstimate(flops=flops, bytes_accessed=16 * rows * width, transcendentals=0),
            name="expert",
        )(near, far, *prepared)

    done = []
    for group in groups:
        parts = lax.optimization_barrier([arrived[s] for s in group] + [crossed[s] for s in group])
        near = jnp.concatenate([p.reshape(local, cap, 2 * width) for p in parts], axis=1)
        far = core(near)
        done.append((near, far, *expert_pass(near, far)))

    sources, returned = [], []
    for g, group in enumerate(groups):
        split = lambda v: v.reshape(local, 2 * len(group), cap, wide)
        near, other = split(done[g][2]), split(core(done[g][5]))
        leaves, owns = sum_group(near, other, tuple(len(u) for u in units[g]))
        for unit, leave, own in zip(units[g], leaves, owns):
            came = chip(leave)
            if unit == (0,):
                sources += [0, 0]
                returned += [own.reshape(slots, wide), came.reshape(slots, wide)]
                continue
            for i, s in enumerate(unit):
                final = (own[:, i].astype(F32) + came[:, i].astype(F32)).astype(BF)
                final = final.reshape(slots, wide)
                sources.append(s)
                returned.append(across(final, s) if s else final)

    near_rows = [d[0] for d in done] + [d[1] for d in done]
    hiddens = [d[3] for d in done] + [d[6] for d in done]
    pres = [d[4] for d in done] + [d[7] for d in done]
    count = len(near_rows)
    steps = 2
    tile = width // steps
    total = sum(r.shape[1] for r in near_rows)

    def weights(step):
        row_specs = [pl.BlockSpec((1, r.shape[1], tile), lambda e: (e, 0, step)) for r in near_rows]
        up_specs = [pl.BlockSpec((1, r.shape[1], tile), lambda e: (e, 0, step + steps)) for r in near_rows]
        hid_specs = [pl.BlockSpec((1, r.shape[1], ff), lambda e: (e, 0, 0)) for r in near_rows]
        pre_specs = [pl.BlockSpec((1, r.shape[1], 2 * ff), lambda e: (e, 0, 0)) for r in near_rows]
        carry = list(grads) if step else []
        return pl.pallas_call(
            functools.partial(weight_kernel, count),
            grid=(local,),
            in_specs=row_specs + up_specs + hid_specs + pre_specs + [pl.BlockSpec(memory_space=pl.ANY)] * len(carry),
            out_specs=[pl.BlockSpec((1, tile, ff), lambda e: (e, step, 0))] * 2
            + [pl.BlockSpec((1, ff, tile), lambda e: (e, 0, step))],
            out_shape=[jax.ShapeDtypeStruct((local, width, ff), BF)] * 2
            + [jax.ShapeDtypeStruct((local, ff, width), BF)],
            scratch_shapes=[pltpu.VMEM((total, n), BF) for n in (tile, tile, ff, 2 * ff)],
            input_output_aliases={4 * count + i: i for i in range(len(carry))},
            compiler_params=limit,
            cost_estimate=pl.CostEstimate(
                flops=2 * local * total * tile * ff * 3, bytes_accessed=local * total * 4 * tile, transcendentals=0
            ),
        )(*near_rows, *near_rows, *hiddens, *pres, *carry)

    grads = None
    for step in range(steps):
        grads = weights(step)
    gate_grad, up_grad, down_grad = grads

    devices = n_dp * n_ctx
    shard = width // devices
    packed = shard % 8 == 0 and shard // 8 * (experts + 1) <= LANES
    lines = 8 if packed else -(-(experts + 1) // 8) * 8
    grad_input, part = pl.pallas_call(
        functools.partial(tail_kernel, local, cap, experts, shard, packed, tuple(sources)),
        out_shape=[jax.ShapeDtypeStruct((rows_here, width), BF), jax.ShapeDtypeStruct((devices, lines, LANES), F32)],
        in_specs=vmem(len(sources) + 7),
        out_specs=vmem(2),
        scratch_shapes=[pltpu.VMEM((LANES, rows_here), F32)],
        compiler_params=limit,
        name="tail",
    )(*returned, rank, gates, tokens, cotangent, labels, norm_gain, router)
    part = lax.all_to_all(part, ("dp", "ctx"), 0, 0, tiled=True)
    if packed:
        grad_router, grad_gain = pl.pallas_call(
            functools.partial(finish_kernel, experts),
            out_shape=[
                jax.ShapeDtypeStruct((shard, experts), F32),
                jax.ShapeDtypeStruct((1, shard), F32),
            ],
            in_specs=vmem(1),
            out_specs=vmem(2),
            name="finish",
        )(part)
        grad_gain = grad_gain.reshape(shard)
    else:
        part = jnp.sum(part, axis=0)
        grad_router, grad_gain = part[:experts, :shard].T, part[experts, :shard]
    return (grad_input, gate_grad, up_grad, down_grad, grad_router, grad_gain)


def solution(mesh):
    return jax.shard_map(
        body,
        mesh=mesh,
        in_specs=(
            P(("dp", "ctx"), None),
            P(("dp", "ctx"), None),
            P(("dp", "ctx"), None),
            P(),
            P(),
            P("ctx", None, "dp"),
            P("ctx", None, "dp"),
            P("ctx", "dp", None),
        ),
        out_specs=(
            P(("dp", "ctx"), None),
            P("ctx", None, "dp"),
            P("ctx", None, "dp"),
            P("ctx", "dp", None),
            P(("dp", "ctx"), None),
            P(("dp", "ctx")),
        ),
        check_vma=False,
    )
```

```python
import functools

import jax
import jax.numpy as jnp
from jax import lax
from jax.experimental import pallas as pl
from jax.experimental.pallas import tpu as pltpu
from jax.sharding import PartitionSpec as P


EPSILON = 1e-05
SWISH_SCALE = 1.702
LANES = 128
BF = jnp.bfloat16
F32 = jnp.float32


def dot(a, b, ca=1, cb=0):
    return lax.dot_general(a, b, (((ca,), (cb,)), ((), ())), preferred_element_type=F32)


def vmem(count):
    return [pl.BlockSpec(memory_space=pltpu.VMEM)] * count


def normalize(tokens_ref, gain_ref):
    widened = tokens_ref[...].astype(F32)
    inverse = lax.rsqrt(jnp.mean(widened * widened, axis=1, keepdims=True) + EPSILON)
    scaled = widened * inverse
    gain = gain_ref[...][None, :]
    return inverse, scaled, (scaled * gain).astype(BF), gain


def permutation(labels_ref, count):
    shape = (labels_ref.shape[0], count)
    return (labels_ref[...] == lax.broadcasted_iota(jnp.int32, shape, 1)).astype(F32).astype(BF)


def slot_mask(table_t, first, local, cap, axis):
    rows = table_t.shape[1 - axis]
    shape = (local * cap, rows) if axis == 0 else (rows, local * cap)
    slot = lax.broadcasted_iota(jnp.int32, shape, axis)
    hit = None
    for e in range(local):
        line = table_t[first + e : first + e + 1, :] if axis == 0 else table_t[:, first + e : first + e + 1]
        one = line == (slot - e * cap).astype(F32)
        one = one & (slot >= e * cap) & (slot < (e + 1) * cap)
        hit = one if hit is None else hit | one
    return hit


def head_kernel(local, cap, tokens_ref, cot_ref, ids_ref, labels_ref, gain_ref, router_ref, *outs):
    messages, (rank_ref, gates_ref) = outs[:-2], outs[-2:]
    rows, width = tokens_ref.shape
    _, _, normed, _ = normalize(tokens_ref, gain_ref)
    router = dot(permutation(labels_ref, router_ref.shape[0]), router_ref[...]).astype(BF)
    logits = dot(router, normed, 1, 1)
    member = None
    for k in range(ids_ref.shape[0]):
        one = ids_ref[k : k + 1, :] == labels_ref[...]
        member = one if member is None else member | one
    lifted = jnp.where(member, jnp.exp(jnp.where(member, logits, 0.0)), 0.0)
    gates_t = lifted / jnp.sum(lifted, axis=0, keepdims=True)
    upto = lax.broadcasted_iota(jnp.int32, (rows, rows), 0) <= lax.broadcasted_iota(jnp.int32, (rows, rows), 1)
    rank_t = dot(member.astype(F32).astype(BF), upto.astype(F32).astype(BF)) - 1.0
    rank_t = jnp.where(member, rank_t, -1.0)
    rank_ref[...] = rank_t
    gates_ref[...] = gates_t
    cot = cot_ref[...]
    for s, out in enumerate(messages):
        hit = slot_mask(rank_t, s * local, local, cap, 0)
        slot = lax.broadcasted_iota(jnp.int32, hit.shape, 0)
        spread = None
        for e in range(local):
            line = gates_t[s * local + e : s * local + e + 1, :]
            part = jnp.where(hit & (slot >= e * cap) & (slot < (e + 1) * cap), line, 0.0)
            spread = part if spread is None else spread + part
        weight = jnp.sum(spread, axis=1, keepdims=True)
        pick = hit.astype(F32).astype(BF)
        out[:, :width] = dot(pick, normed).astype(BF)
        out[:, width:] = (dot(pick, cot) * weight).astype(BF)


def prepare_kernel(gate_ref, up_ref, down_ref, both_ref, turned_ref, down_out):
    ff = gate_ref.shape[2]
    both_ref[0, :, :ff] = gate_ref[0]
    both_ref[0, :, ff:] = up_ref[0]
    turned_ref[0, :ff, :] = gate_ref[0].T
    turned_ref[0, ff:, :] = up_ref[0].T
    down_out[0] = down_ref[0].T


def expert_kernel(width, near_ref, far_ref, both_ref, turned_ref, down_ref, *outs):
    both, turned, down = both_ref[0], turned_ref[0], down_ref[0]
    ff = down.shape[1]
    for rows_ref, (back_ref, hidden_ref, pre_ref) in ((near_ref, outs[:3]), (far_ref, outs[3:])):
        pre = dot(rows_ref[0, :, :width], both)
        gate_pre, up_one = pre[:, :ff], pre[:, ff:] + 1.0
        grad = dot(rows_ref[0, :, width:], down)
        squash = jax.nn.sigmoid(SWISH_SCALE * gate_pre)
        swish = gate_pre * squash
        hidden = (swish * up_one).astype(BF)
        score = jnp.sum(grad * hidden.astype(F32), axis=1, keepdims=True)
        slope = squash + SWISH_SCALE * swish * (1.0 - squash)
        hidden_ref[0] = hidden
        pre_ref[0, :, :ff] = (grad * up_one * slope).astype(BF)
        pre_ref[0, :, ff:] = (grad * swish).astype(BF)
        back_ref[0, :, :width] = dot(pre_ref[0], turned).astype(BF)
        lane = lax.broadcasted_iota(jnp.int32, (score.shape[0], LANES), 1)
        back_ref[0, :, width:] = jnp.where(lane == 0, score, 0.0).astype(BF)


def weight_kernel(count, *refs):
    gate_out, up_out, down_out, rows_ref, ups_ref, hid_ref, pre_ref = refs[-7:]
    ff = gate_out.shape[2]
    for n, joined in enumerate((rows_ref, ups_ref, hid_ref, pre_ref)):
        at = 0
        for piece in refs[n * count : (n + 1) * count]:
            joined[at : at + piece.shape[1]] = piece[0]
            at += piece.shape[1]
    both = dot(rows_ref[...], pre_ref[...], 0, 0)
    gate_out[0] = both[:, :ff].astype(BF)
    up_out[0] = both[:, ff:].astype(BF)
    down_out[0] = dot(hid_ref[...], ups_ref[...], 0, 0).astype(BF)


def tail_kernel(local, cap, experts, shard, packed, sources, *refs):
    count = len(sources)
    pieces = refs[:count]
    rank_ref, gates_ref, tokens_ref, cot_ref, labels_ref, gain_ref, router_ref = refs[count : count + 7]
    grad_ref, part_ref, score_ref = refs[count + 7 :]
    width = tokens_ref.shape[1]
    rank_t = rank_ref[...]
    rank = rank_t.T
    inverse, scaled, normed, gain = normalize(tokens_ref, gain_ref)
    router = dot(permutation(labels_ref, experts), router_ref[...]).astype(BF)
    score_ref[...] = jnp.zeros(score_ref.shape, F32)
    back = None
    for s, piece in zip(sources, pieces):
        pick = slot_mask(rank, s * local, local, cap, 1).astype(F32).astype(BF)
        part = dot(pick, piece[:, :width])
        back = part if back is None else back + part
        column = piece[:, width : width + LANES].astype(F32)[:, :1]
        hit = slot_mask(rank_t, s * local, local, cap, 0)
        slot = lax.broadcasted_iota(jnp.int32, hit.shape, 0)
        for e in range(local):
            mine = hit & (slot >= e * cap) & (slot < (e + 1) * cap)
            score_ref[s * local + e : s * local + e + 1, :] += jnp.sum(
                jnp.where(mine, column, 0.0), axis=0, keepdims=True
            )
    score = score_ref[...]
    mixed = jnp.sum(score, axis=0, keepdims=True)
    grad_logits = jnp.where(rank_t >= 0.0, score - gates_ref[...] * mixed, 0.0)
    grad_normed = back + dot(grad_logits.T.astype(BF), router)
    natural = dot(permutation(labels_ref, LANES), grad_logits.astype(BF), 0, 0)
    part_t = dot(natural.astype(BF), normed)
    gain_part = jnp.sum(grad_normed * scaled, axis=0, keepdims=True)
    line = lax.broadcasted_iota(jnp.int32, (LANES, width), 0)
    part = jnp.where(line == experts, gain_part, part_t)
    if packed:
        columns = part.T
        for d in range(part_ref.shape[0]):
            first = d * shard
            total = columns[first : first + 8]
            for g in range(1, shard // 8):
                total = total + pltpu.roll(columns[first + 8 * g : first + 8 * g + 8], g * (experts + 1), 1)
            part_ref[d] = total
    else:
        part_ref[...] = jnp.zeros(part_ref.shape, F32)
        for d in range(part_ref.shape[0]):
            part_ref[d, :, :shard] = part[: part_ref.shape[1], d * shard : (d + 1) * shard]
    grad_scaled = grad_normed * gain
    correction = jnp.mean(grad_scaled * scaled, axis=1, keepdims=True)
    grad_ref[...] = (
        cot_ref[...].astype(F32) + inverse * (grad_scaled - scaled * correction)
    ).astype(BF)


def sum_group(near, other, sizes):
    count = near.shape[1] // 2
    leaves, owns, at = [], [], 0
    for size in sizes:
        for out, first in ((leaves, count + at), (owns, at)):
            cut = slice(first, first + size)
            out.append((near[:, cut].astype(F32) + other[:, cut].astype(F32)).astype(BF))
        at += size
    return lax.optimization_barrier((leaves, owns))


def finish_kernel(experts, in_ref, router_ref, gain_ref):
    total = jnp.sum(in_ref[...], axis=0)
    turned = jnp.concatenate([total] * (LANES // 8), axis=0).T
    for g in range(gain_ref.shape[1] // 8):
        first = g * (experts + 1)
        lanes = slice(8 * g, 8 * g + 8)
        router_ref[:, lanes] = turned[first : first + experts, lanes]
        gain_ref[:, lanes] = turned[first + experts : first + experts + 1, lanes]


def plan(n_ctx):
    if n_ctx == 8:
        return ((0, 1, 2, 4), (3, 5), (6, 7)), (((0,), (1, 2), (4,)), ((3,), (5,)), ((6,), (7,)))
    half, quarter = n_ctx // 2, n_ctx // 4
    groups = (tuple(range(half)), tuple(range(half, half + quarter)), tuple(range(half + quarter, n_ctx)))
    return groups, tuple((g,) for g in groups)


def body(tokens, cotangent, expert_ids, norm_gain, router_weight, gate_weight, up_weight, down_weight):
    n_ctx, n_dp = lax.axis_size("ctx"), lax.axis_size("dp")
    me = lax.axis_index("ctx")
    local, width, ff = gate_weight.shape
    experts = router_weight.shape[1]
    rows_here, picks = expert_ids.shape
    cap = max(2, rows_here * picks * 5 // (4 * experts))
    slots = local * cap
    wide = width + LANES
    labels = jnp.arange(experts, dtype=jnp.int32)
    labels = ((labels // local) ^ me) * local + labels % local
    labels = jnp.pad(labels, (0, LANES - experts), constant_values=-1)[:, None]
    router = router_weight.T
    limit = pltpu.CompilerParams(vmem_limit_bytes=56 * 1024 * 1024)

    *messages, rank, gates = pl.pallas_call(
        functools.partial(head_kernel, local, cap),
        out_shape=[jax.ShapeDtypeStruct((slots, 2 * width), BF)] * n_ctx
        + [jax.ShapeDtypeStruct((rows_here, LANES), F32)] * 2,
        in_specs=vmem(6),
        out_specs=vmem(n_ctx + 2),
        compiler_params=limit,
        name="head",
    )(tokens, cotangent, expert_ids.T, labels, norm_gain, router)

    def across(value, s):
        return lax.ppermute(value, "ctx", [(i, i ^ s) for i in range(n_ctx)])

    def chip(value):
        return lax.ppermute(value, "dp", [(i, i ^ 2) for i in range(n_dp)])

    def core(value):
        return lax.ppermute(value, "dp", [(i, i ^ 1) for i in range(n_dp)])

    groups, units = plan(n_ctx)
    arrived = {s: across(messages[s], s) if s else messages[s] for s in range(n_ctx)}
    crossed = {s: chip(arrived[s]) for s in range(n_ctx)}

    turn = lambda *shape: pl.BlockSpec((1, *shape), lambda e: (e, 0, 0))
    turned_shapes = ((width, 2 * ff), (2 * ff, width), (width, ff))
    prepared = pl.pallas_call(
        prepare_kernel,
        grid=(local,),
        in_specs=[turn(width, ff)] * 2 + [turn(ff, width)],
        out_specs=[turn(*t) for t in turned_shapes],
        out_shape=[jax.ShapeDtypeStruct((local, *t), BF) for t in turned_shapes],
        compiler_params=limit,
        name="prepare",
    )(gate_weight, up_weight, down_weight)

    def expert_pass(near, far):
        rows = near.shape[1]
        spec = lambda *shape: pl.BlockSpec((1, *shape), lambda e: (e, 0, 0))
        outs = ((rows, wide), (rows, ff), (rows, 2 * ff)) * 2
        flops = 2 * 2 * local * rows * width * ff * 5
        return pl.pallas_call(
            functools.partial(expert_kernel, width),
            grid=(local,),
            in_specs=[spec(rows, 2 * width)] * 2 + [spec(width, 2 * ff), spec(2 * ff, width), spec(width, ff)],
            out_specs=[spec(*o) for o in outs],
            out_shape=[jax.ShapeDtypeStruct((local, *o), BF) for o in outs],
            compiler_params=limit,
            cost_estimate=pl.CostEstimate(flops=flops, bytes_accessed=16 * rows * width, transcendentals=0),
            name="expert",
        )(near, far, *prepared)

    done = []
    for group in groups:
        parts = lax.optimization_barrier([arrived[s] for s in group] + [crossed[s] for s in group])
        near = jnp.concatenate([p.reshape(local, cap, 2 * width) for p in parts], axis=1)
        far = core(near)
        done.append((near, far, *expert_pass(near, far)))

    sources, returned = [], []
    for g, group in enumerate(groups):
        split = lambda v: v.reshape(local, 2 * len(group), cap, wide)
        near, other = split(done[g][2]), split(core(done[g][5]))
        leaves, owns = sum_group(near, other, tuple(len(u) for u in units[g]))
        for unit, leave, own in zip(units[g], leaves, owns):
            came = chip(leave)
            if unit == (0,):
                sources += [0, 0]
                returned += [own.reshape(slots, wide), came.reshape(slots, wide)]
                continue
            for i, s in enumerate(unit):
                final = (own[:, i].astype(F32) + came[:, i].astype(F32)).astype(BF)
                final = final.reshape(slots, wide)
                sources.append(s)
                returned.append(across(final, s) if s else final)

    near_rows = [d[0] for d in done] + [d[1] for d in done]
    hiddens = [d[3] for d in done] + [d[6] for d in done]
    pres = [d[4] for d in done] + [d[7] for d in done]
    count = len(near_rows)
    steps = 2
    tile = width // steps
    total = sum(r.shape[1] for r in near_rows)

    def weights(step):
        row_specs = [pl.BlockSpec((1, r.shape[1], tile), lambda e: (e, 0, step)) for r in near_rows]
        up_specs = [pl.BlockSpec((1, r.shape[1], tile), lambda e: (e, 0, step + steps)) for r in near_rows]
        hid_specs = [pl.BlockSpec((1, r.shape[1], ff), lambda e: (e, 0, 0)) for r in near_rows]
        pre_specs = [pl.BlockSpec((1, r.shape[1], 2 * ff), lambda e: (e, 0, 0)) for r in near_rows]
        carry = list(grads) if step else []
        return pl.pallas_call(
            functools.partial(weight_kernel, count),
            grid=(local,),
            in_specs=row_specs + up_specs + hid_specs + pre_specs + [pl.BlockSpec(memory_space=pl.ANY)] * len(carry),
            out_specs=[pl.BlockSpec((1, tile, ff), lambda e: (e, step, 0))] * 2
            + [pl.BlockSpec((1, ff, tile), lambda e: (e, 0, step))],
            out_shape=[jax.ShapeDtypeStruct((local, width, ff), BF)] * 2
            + [jax.ShapeDtypeStruct((local, ff, width), BF)],
            scratch_shapes=[pltpu.VMEM((total, n), BF) for n in (tile, tile, ff, 2 * ff)],
            input_output_aliases={4 * count + i: i for i in range(len(carry))},
            compiler_params=limit,
            cost_estimate=pl.CostEstimate(
                flops=2 * local * total * tile * ff * 3, bytes_accessed=local * total * 4 * tile, transcendentals=0
            ),
        )(*near_rows, *near_rows, *hiddens, *pres, *carry)

    grads = None
    for step in range(steps):
        grads = weights(step)
    gate_grad, up_grad, down_grad = grads

    devices = n_dp * n_ctx
    shard = width // devices
    packed = shard % 8 == 0 and shard // 8 * (experts + 1) <= LANES
    lines = 8 if packed else -(-(experts + 1) // 8) * 8
    grad_input, part = pl.pallas_call(
        functools.partial(tail_kernel, local, cap, experts, shard, packed, tuple(sources)),
        out_shape=[jax.ShapeDtypeStruct((rows_here, width), BF), jax.ShapeDtypeStruct((devices, lines, LANES), F32)],
        in_specs=vmem(len(sources) + 7),
        out_specs=vmem(2),
        scratch_shapes=[pltpu.VMEM((LANES, rows_here), F32)],
        compiler_params=limit,
        name="tail",
    )(*returned, rank, gates, tokens, cotangent, labels, norm_gain, router)
    part = lax.all_to_all(part, ("dp", "ctx"), 0, 0, tiled=True)
    if packed:
        grad_router, grad_gain = pl.pallas_call(
            functools.partial(finish_kernel, experts),
            out_shape=[
                jax.ShapeDtypeStruct((experts, shard), F32),
                jax.ShapeDtypeStruct((1, shard), F32),
            ],
            in_specs=vmem(1),
            out_specs=vmem(2),
            name="finish",
        )(part)
        grad_router, grad_gain = grad_router.T, grad_gain.reshape(shard)
    else:
        part = jnp.sum(part, axis=0)
        grad_router, grad_gain = part[:experts, :shard].T, part[experts, :shard]
    return (grad_input, gate_grad, up_grad, down_grad, grad_router, grad_gain)


def solution(mesh):
    return jax.shard_map(
        body,
        mesh=mesh,
        in_specs=(
            P(("dp", "ctx"), None),
            P(("dp", "ctx"), None),
            P(("dp", "ctx"), None),
            P(),
            P(),
            P("ctx", None, "dp"),
            P("ctx", None, "dp"),
            P("ctx", "dp", None),
        ),
        out_specs=(
            P(("dp", "ctx"), None),
            P("ctx", None, "dp"),
            P("ctx", None, "dp"),
            P("ctx", "dp", None),
            P(("dp", "ctx"), None),
            P(("dp", "ctx")),
        ),
        check_vma=False,
    )
```
